32 devices in a mesh: dp: 4 (over z), row: 2 (over x), col: 4 (over y, core).
Axes of the slice: x: 2, y: 2, z: 4, core: 2. Of those that a mesh axis runs over, the one named last changes fastest.
Arguments:
- grad: bfloat16 [4, 4096, 14336], P('dp', 'row', 'col'), may hold values from -6 to 6
- error: bfloat16 [4, 4096, 14336], P('dp', 'row', 'col'), may hold values from -6 to 6
- q_init: float32 [14336, 128], P('col'), may hold values from -6 to 6
Outputs:
- new_error: bfloat16 [4, 4096, 14336], P('dp', 'row', 'col')
- q_factor: float32 [14336, 128], P('col')
The draws below stay inside these ranges and needn't reach their ends.
All inputs are finite; a program needn't handle non-finite values.
Results may differ from the reference program's by a relative error of at most 0.001.
Values sent between devices are 32-bit elements; how exact they have to be, the bound alone decides.
A program may use at most 128 MiB of HBM per device.

```python
import jax
import jax.numpy as jnp
from jax import lax

ROWS = 4096
COLS = 14336
RANK = 128
ITERS = 2
N_DP = 4


def block_scale(key, shape, cuts, smallest, largest):
    gain = 1.0
    for position, shards_of in cuts:
        heights = jax.random.uniform(jax.random.fold_in(jax.random.fold_in(key, 6), position), (shards_of,), jnp.float32, smallest / len(cuts), largest / len(cuts))
        gain = gain * jnp.repeat(jnp.exp(heights), shape[position] // shards_of).reshape((-1,) + (1,) * (len(shape) - 1 - position))
    return gain


def gaussian(key, dims, width, bound, shards=(), kind=jnp.bfloat16):
    level = block_scale(key, dims, shards, -0.22, 0.18) if shards else 1.0
    array = jax.random.normal(key, dims, jnp.float32) * width * level
    return jnp.minimum(jnp.maximum(array, -bound), bound).astype(kind)


def setup_inputs(seed: int = 0) -> dict:
    keys = jax.random.split(jax.random.key(seed), 4)
    grad = gaussian(keys[0], (N_DP, ROWS, COLS), 1.0, 6.0, ((0, 4), (1, 2), (2, 4)))
    error = gaussian(keys[1], (N_DP, ROWS, COLS), 0.5, 6.0, ((0, 4), (1, 2), (2, 4)))
    q_init = gaussian(keys[2], (COLS, RANK), 1.0, 6.0, ((0, 4),), jnp.float32)
    return dict(grad=grad, error=error, q_init=q_init)


def orthonormal(p_mat):
    gram = jnp.dot(p_mat.T.astype(jnp.float32), p_mat.astype(jnp.float32), precision=lax.Precision.HIGHEST, preferred_element_type=jnp.float32)
    lower = jnp.linalg.cholesky(gram)
    return jax.scipy.linalg.solve_triangular(lower, p_mat.T, lower=True).T

def reference(grad, error, q_init):
    workers = grad.shape[0]
    q_mat = q_init
    p_hat = None
    for step in range(ITERS):
        p_mat = jnp.zeros((grad.shape[1], q_mat.shape[1]), jnp.float32)
        for worker in range(workers):
            comp = grad[worker].astype(jnp.float32) + error[worker].astype(jnp.float32)
            p_mat = p_mat + jnp.dot(comp.astype(jnp.float32), q_mat.astype(jnp.float32), precision=lax.Precision.HIGHEST, preferred_element_type=jnp.float32)
        p_hat = orthonormal(p_mat * (1.0 / workers))
        q_next = jnp.zeros(q_mat.shape, jnp.float32)
        for worker in range(workers):
            comp = grad[worker].astype(jnp.float32) + error[worker].astype(jnp.float32)
            q_next = q_next + jnp.dot(comp.T.astype(jnp.float32), p_hat.astype(jnp.float32), precision=lax.Precision.HIGHEST, preferred_element_type=jnp.float32)
        q_mat = q_next * (1.0 / workers)
    approx = jnp.dot(p_hat.astype(jnp.float32), q_mat.T.astype(jnp.float32), precision=lax.Precision.HIGHEST, preferred_element_type=jnp.float32)
    comp_all = grad.astype(jnp.float32) + error.astype(jnp.float32)
    new_error = (comp_all - approx[None]).astype(jnp.bfloat16)
    return (new_error, q_mat)
```

```python
import jax
import jax.numpy as jnp
from jax import lax
from jax.sharding import PartitionSpec as P

ITERS = 2


def power_of_two(n):
    return n & (n - 1) == 0


def exchange(value, axis, bit):
    n = lax.axis_size(axis)
    return lax.ppermute(value, axis, [(i, i ^ bit) for i in range(n)])


def bits_of(axes):
    steps = []
    for axis in axes:
        bit = 1
        while bit < lax.axis_size(axis):
            steps.append((axis, bit))
            bit *= 2
    return steps


def upper(axis, bit):
    return lax.rem(lax.axis_index(axis) // bit, 2)


def butterfly(values_axes):
    state = [(value, bits_of(axes)) for value, axes in values_axes]
    values = [value for value, _ in state]
    depth = len(state[0][1])
    for level in range(depth):
        for k, (_, steps) in enumerate(state):
            axis, bit = steps[level]
            half = values[k].shape[0] // 2
            side = upper(axis, bit)
            keep = lax.dynamic_slice_in_dim(values[k], side * half, half, 0)
            give = lax.dynamic_slice_in_dim(values[k], (1 - side) * half, half, 0)
            values[k] = keep + exchange(give, axis, bit)
    for level in reversed(range(depth)):
        for k, (_, steps) in enumerate(state):
            axis, bit = steps[level]
            first = upper(axis, bit) == 0
            mine = values[k]
            other = exchange(mine, axis, bit)
            values[k] = jnp.concatenate(
                [jnp.where(first, mine, other), jnp.where(first, other, mine)], axis=0
            )
    return values


def reduce_over(value, axis_a, axis_b):
    sizes = lax.axis_size(axis_a), lax.axis_size(axis_b)
    rows = value.shape[0]
    if not all(map(power_of_two, sizes)) or rows % (2 * sizes[0] * sizes[1]):
        return lax.psum(value, (axis_a, axis_b))
    half = rows // 2
    parts = butterfly(
        [(value[:half], (axis_a, axis_b)), (value[half:], (axis_b, axis_a))]
    )
    return jnp.concatenate(parts, axis=0)


def reduce_small(value, axis):
    if not power_of_two(lax.axis_size(axis)):
        return lax.psum(value, axis)
    for name, bit in bits_of((axis,)):
        value = value + exchange(value, name, bit)
    return value


def split(value):
    high = lax.reduce_precision(value, exponent_bits=8, mantissa_bits=7)
    return high.astype(jnp.bfloat16), (value - high).astype(jnp.bfloat16)


def product(high, low, factor, side):
    rank = factor.shape[1]
    both = jnp.concatenate(split(factor), axis=1)
    dims = (((side,), (0,)), ((), ()))
    total = lax.dot_general(high, both, dims, preferred_element_type=jnp.float32)
    total = total + lax.dot_general(low, both, dims, preferred_element_type=jnp.float32)
    return total[:, :rank] + total[:, rank:]


def exact_dot(a, b, dims):
    return lax.dot_general(
        a, b, (dims, ((), ())), precision=lax.Precision.HIGHEST,
        preferred_element_type=jnp.float32,
    )


def shards(grad, error, q_init):
    comp = grad[0].astype(jnp.float32) + error[0].astype(jnp.float32)
    high, low = lax.optimization_barrier(split(comp))
    scale = 1.0 / lax.axis_size("dp")
    q_mat = q_init
    p_hat = None
    eye = jnp.eye(q_init.shape[1], dtype=jnp.float32)
    for step in range(ITERS):
        p_mat = reduce_over(product(high, low, q_mat, 1), "col", "dp") * scale
        gram = reduce_small(exact_dot(p_mat, p_mat, ((0,), (0,))), "row")
        term = reduce_over(product(high, low, p_mat, 0), "row", "dp") * scale
        lower = jnp.linalg.cholesky(gram)
        inverse = jax.scipy.linalg.solve_triangular(lower, eye, lower=True)
        q_mat = exact_dot(term, inverse, ((1,), (1,)))
        p_hat = exact_dot(p_mat, inverse, ((1,), (1,)))
    p_high, p_low = split(p_hat)
    q_high, q_low = split(q_mat)
    left = jnp.concatenate([p_high, p_high, p_low], axis=1)
    right = jnp.concatenate([q_high, q_low, q_high], axis=1)
    approx = lax.dot_general(
        left, right, (((1,), (1,)), ((), ())), preferred_element_type=jnp.float32
    )
    comp = grad[0].astype(jnp.float32) + error[0].astype(jnp.float32)
    new_error = (comp - approx).astype(jnp.bfloat16)[None]
    return (new_error, q_mat)


def solution(mesh):
    in_specs = (P("dp", "row", "col"), P("dp", "row", "col"), P("col", None))
    out_specs = (P("dp", "row", "col"), P("col", None))
    return jax.shard_map(shards, mesh=mesh, in_specs=in_specs, out_specs=out_specs, check_vma=False)
```
